32 devices in a mesh: gx: 4 (over z), gy: 8 (over y, x, core).
Axes of the slice: x: 2, y: 2, z: 4, core: 2. Of those that a mesh axis runs over, the one named last changes fastest.
Arguments:
- item_table: bfloat16 [262144, 256], P(('gx', 'gy')), may hold values from -0.625 to 0.625
- bilinear: bfloat16 [256, 1024], replicated, may hold values from -0.375 to 0.375
- requests: int32 [32, 32, 64], P(('gx', 'gy')), may hold values from -1 to 8191, as said below
- history: int32 [8192, 50], P(('gx', 'gy')), may hold values from 0 to 2047, as said below
- lengths: int32 [8192], P(('gx', 'gy')), may hold values from 10 to 50
- init_logits: float32 [8192, 50, 4], P(('gx', 'gy')), may hold values from -6 to 6
- interest_grad: float32 [8192, 4, 256], P(('gx', 'gy')), may hold values from -6 to 6
Outputs:
- interests: bfloat16 [8192, 4, 256], P(('gx', 'gy'))
- table_grad: float32 [262144, 256], P(('gx', 'gy'))
The draws below stay inside these ranges and needn't reach their ends.
Inputs may be any that keep to these rules, and one draw needn't show every extreme that they name: requests[r, o, c] is a row of table shard o asked by device r in slot c, or -1 for an unused slot; the used slots of a list come first, hold distinct rows, and number at least one; a few shards have full lists (64 used slots) from every device. history[u, l] = o * 64 + c names a used slot c of list o of the device holding user u (users are laid out 256 a device).
All inputs are finite; a program needn't handle non-finite values.
Results may differ from the reference program's by a relative error of at most 0.015.
Values may be sent and summed in bfloat16 or wider, within the bound.
No kernel may reach another device: no remote copies, remote signals or barrier semaphores. Data moves between devices by JAX's collectives and lax.ppermute only.
A program may use at most 192 MiB of HBM per device.

```python
import jax
import jax.numpy as jnp
from jax import lax

D = 256
INTERESTS = 4
HIST_LEN = 50
ITERS = 3
ROWS_DEV = 8192
CAP = 64
USERS_DEV = 256
OWNERS = 32
USERS = 8192
ITEMS = 262144


def request_layout(key):
    keys = jax.random.split(jax.random.fold_in(key, 11), 5)
    popular = jax.random.permutation(keys[0], OWNERS) < 4
    drawn = jax.random.randint(keys[1], (OWNERS, OWNERS), CAP // 2, CAP + 1)
    counts = jnp.where(popular[None, :], CAP, drawn).astype(jnp.int32)
    offset = jax.random.randint(keys[2], (OWNERS, OWNERS, 1), 0, ROWS_DEV)
    stride = 2 * jax.random.randint(keys[3], (OWNERS, OWNERS, 1), 0, ROWS_DEV // 2) + 1
    slot_ids = jnp.arange(CAP, dtype=jnp.int32)[None, None, :]
    asked_rows = (offset + slot_ids * stride) % ROWS_DEV
    requests = jnp.where(slot_ids < counts[:, :, None], asked_rows, -1).astype(jnp.int32)
    totals = jnp.sum(counts, axis=1)
    ends = jnp.cumsum(counts, axis=1)
    starts = ends - counts
    picks = jax.random.randint(keys[4], (OWNERS, USERS_DEV * HIST_LEN), 0, totals[:, None])
    owner_ids = jax.vmap(lambda edge, value: jnp.searchsorted(edge, value, side='right'))(ends, picks).astype(jnp.int32)
    ranks = picks - jnp.take_along_axis(starts, owner_ids, axis=1)
    history = (owner_ids * CAP + ranks).astype(jnp.int32).reshape(OWNERS * USERS_DEV, HIST_LEN)
    return (requests, history)


def draw_requests(key, part):
    return request_layout(key)[0]


def draw_history(key, part):
    return request_layout(key)[1]


def touch_ends(array, stream_key, smallest, largest):
    shape = array.shape
    spot = [jax.random.randint(jax.random.fold_in(stream_key, axis), (), 0, shape[axis]) for axis in range(len(shape))]
    array = array.at[tuple(spot)].set(smallest)
    longest = shape.index(max(shape))
    spot[longest] = (spot[longest] + 1) % shape[longest]
    return array.at[tuple(spot)].set(largest)


def steps_of(rng, extent, shards, low, high):
    gain = 1.0
    for axis_at, blocks in shards:
        steps = jax.random.uniform(jax.random.fold_in(jax.random.fold_in(rng, 6), axis_at), (blocks,), jnp.float32, low / len(shards), high / len(shards))
        gain = gain * jnp.repeat(jnp.exp(steps), extent[axis_at] // blocks).reshape((-1,) + (1,) * (len(extent) - 1 - axis_at))
    return gain


def normal_values(stream_key, shape, deviation, most, pieces=(), kind=jnp.bfloat16):
    values = jax.random.normal(stream_key, shape, jnp.float32) * deviation
    if len(pieces) > 0:
        values = steps_of(stream_key, shape, pieces, -0.22, 0.18) * values
    return jnp.clip(values, min=-most, max=most).astype(kind)


def setup_inputs(seed: int = 0) -> dict:
    key_list = jax.random.split(jax.random.key(seed), 8)
    return {
        "item_table": normal_values(key_list[0], (ITEMS, D), 0.1, 0.625, ((0, 32),)),
        "bilinear": normal_values(key_list[1], (D, INTERESTS * D), D ** -0.5, 0.375),
        "requests": draw_requests(jax.random.fold_in(key_list[7], 71), 0),
        "history": draw_history(jax.random.fold_in(key_list[7], 71), 0),
        "lengths": touch_ends(jax.random.randint(key_list[4], (USERS,), max(1, HIST_LEN // 5), HIST_LEN + 1), jax.random.fold_in(key_list[4], 1), max(1, HIST_LEN // 5), HIST_LEN).astype(jnp.int32),
        "init_logits": normal_values(key_list[5], (USERS, HIST_LEN, INTERESTS), 1.0, 6.0, ((0, 32),), jnp.float32),
        "interest_grad": normal_values(key_list[6], (USERS, INTERESTS, D), 1.0, 6.0, ((0, 32),), jnp.float32),
    }


squash_eps = 1e-06

def route_interests(behavior_rows, bilinear, lengths, init_logits):
    users_here, hist_count, feature_width = behavior_rows.shape
    interest_count = init_logits.shape[2]
    remapped_values = jnp.dot(behavior_rows.reshape(users_here * hist_count, feature_width), bilinear, preferred_element_type=jnp.float32)
    remapped_values = remapped_values.astype(jnp.bfloat16).reshape(users_here, hist_count, interest_count, feature_width)
    positions = lax.broadcasted_iota(jnp.int32, (users_here, hist_count), 1)
    live_mask = (positions < lengths[:, None]).astype(jnp.float32)
    logits = init_logits
    interest_capsule = None
    for turn_no in range(ITERS):
        exponent = jnp.exp(logits)
        coupling_weight = exponent / lax.optimization_barrier(jnp.sum(exponent, axis=2, keepdims=True)) * live_mask[:, :, None]
        weighted_total = jnp.einsum('rmq,rmqs->rqs', coupling_weight.astype(jnp.bfloat16), remapped_values, preferred_element_type=jnp.float32)
        norm_sq = lax.optimization_barrier(jnp.sum(weighted_total * weighted_total, axis=2, keepdims=True))
        interest_capsule = weighted_total * jnp.sqrt(norm_sq + squash_eps) / (1.0 + norm_sq)
        if turn_no + 1 < ITERS:
            routing_agreement_score = jnp.einsum('mazc,mzc->maz', remapped_values, interest_capsule.astype(jnp.bfloat16), preferred_element_type=jnp.float32)
            logits = logits + routing_agreement_score
    return interest_capsule

def reference(item_table, bilinear, requests, history, lengths, init_logits, interest_grad):
    feature_width = item_table.shape[1]
    flattened_request_list = requests.reshape(OWNERS, OWNERS * CAP)

    def per_device(carried, block_no):
        start = block_no * USERS_DEV
        history_item_block = lax.dynamic_slice_in_dim(history, start, USERS_DEV, 0)
        length_block = lax.dynamic_slice_in_dim(lengths, start, USERS_DEV, 0)
        logit_block = lax.dynamic_slice_in_dim(init_logits, start, USERS_DEV, 0)
        grad_block = lax.dynamic_slice_in_dim(interest_grad, start, USERS_DEV, 0)
        own_list = lax.dynamic_index_in_dim(flattened_request_list, block_no, 0, keepdims=False)
        local_table_rows = jnp.take(own_list, history_item_block.reshape(-1), axis=0)
        item_ids = (history_item_block.reshape(-1) // CAP * ROWS_DEV + local_table_rows).astype(jnp.int32)
        behavior_rows = jnp.take(item_table, item_ids, axis=0).reshape(USERS_DEV, HIST_LEN, feature_width)
        interest_capsule, pullback = jax.vjp(lambda given: route_interests(given, bilinear, length_block, logit_block), behavior_rows)
        row_grad, = pullback(grad_block)
        carried = carried.at[item_ids].add(row_grad.reshape(-1, feature_width).astype(jnp.float32))
        return (carried, interest_capsule.astype(jnp.bfloat16))
    empty = jnp.zeros((ITEMS, feature_width), jnp.float32)
    table_grad, capsules = lax.scan(per_device, empty, jnp.arange(OWNERS, dtype=jnp.int32))
    return (capsules.reshape(USERS, INTERESTS, feature_width), table_grad)
```

```python
import functools

import jax
import jax.numpy as jnp
from jax import lax
from jax.experimental import pallas as pl
from jax.experimental.pallas import tpu as pltpu
from jax.sharding import PartitionSpec as P

ITERS = 3
squash_eps = 1e-06
AXES = ("gx", "gy")
BLOCK_USERS = 64
TILE_POSITIONS = 4
f32 = jnp.float32
bf16 = jnp.bfloat16


def dot(a, b):
    return jnp.dot(a, b, preferred_element_type=f32)


def routing_kernel(
    interest_count, tile_count,
    fetched_ref, bil_ref, bilt_ref, owner_ref, slot_ref, lens_ref, logit_ref, cot_ref,
    interests_ref, slotgrad_ref,
    fetched_t, x_ref, xt_ref, lo_ref, oht_a, oht_b, mcat, vcat, stack, rg_ref, oh_rows, rows_a, slot_acc,
):
    slots, width = fetched_ref.shape
    tiles, lanes = owner_ref.shape
    block_count = tiles // tile_count
    cap = lo_ref.shape[1]
    owners = slots // cap
    users = BLOCK_USERS

    for c in range(0, slots, 256):
        fetched_t[:, c:c + 256] = fetched_ref[c:c + 256, :].T

    slot_iota = lax.broadcasted_iota(jnp.int32, (cap, lanes), 0)

    def indicator(orow16, o):
        return jnp.where(orow16 == o, 1.0, 0.0).astype(bf16)

    def build(tile, buf):
        crow = slot_ref[pl.ds(tile, 1), :]
        orow16 = jnp.broadcast_to(owner_ref[pl.ds(tile, 1), :], (16, lanes))
        lo = jnp.where(slot_iota == crow, 1.0, 0.0).astype(bf16)
        lo_ref[tile] = lo
        lo3 = lo.reshape(cap // 16, 16, lanes)

        for o in range(owners):
            buf[o * cap:(o + 1) * cap, :] = (lo3 * indicator(orow16, o)[None]).reshape(cap, lanes)

    def gather(tile, buf):
        xt = dot(fetched_t[...], buf[...])
        xtb = xt.astype(bf16)
        xt_ref[tile] = xtb
        x_ref[tile] = xtb.T

    build(0, oht_a)

    def gather_pair(i, carry):
        t = 2 * i
        build(t + 1, oht_b)
        gather(t, oht_a)
        build(jnp.minimum(t + 2, tiles - 1), oht_a)
        gather(t + 1, oht_b)
        return carry

    lax.fori_loop(0, tiles // 2, gather_pair, 0)

    row_iota = lax.broadcasted_iota(jnp.int32, (users, lanes), 0)
    lane_iota = lax.broadcasted_iota(jnp.int32, (users, lanes), 1)
    diag = (lane_iota % users) == row_iota
    lane_k = lax.broadcasted_iota(jnp.int32, (width, lanes), 1) // users
    padded = logit_ref.shape[1]
    half = lanes // 2

    def over_interests(v):
        s = v[:, :half] + v[:, half:]
        s = s + pltpu.roll(s, users, 1)
        return jnp.concatenate([s, s], axis=1)

    def spread(coef, j):
        rows_a[...] = coef
        for l in range(tile_count * TILE_POSITIONS):
            row = jnp.broadcast_to(rows_a[l:l + 1, :], (users, lanes))
            mcat[l * users:(l + 1) * users, j * lanes:(j + 1) * lanes] = jnp.where(diag, row, 0.0).astype(bf16)

    def weighted_sum(b, j):
        total = jnp.zeros((width, lanes), f32)
        for t in range(tile_count):
            total = total + dot(
                xt_ref[b * tile_count + t],
                mcat[t * lanes:(t + 1) * lanes, j * lanes:(j + 1) * lanes],
            )
        return total

    def agreement(b, vec):
        for t in range(tile_count):
            prod = dot(x_ref[b * tile_count + t], vec)
            for p in range(TILE_POSITIONS):
                part = jnp.where(diag, prod[p * users:(p + 1) * users, :], 0.0)
                l = t * TILE_POSITIONS + p
                rows_a[l:l + 1, :] = jnp.sum(part, axis=0, keepdims=True)
        return rows_a[...]

    def by_interest(mat_ref, v):
        vb = v.astype(bf16)
        zero = jnp.zeros_like(v)
        for k in range(interest_count):
            stack[k * width:(k + 1) * width, :] = jnp.where(lane_k == k, v, zero).astype(bf16)
        return dot(mat_ref[...], stack[...])

    def squash(s):
        n = jnp.sum(s * s, axis=0, keepdims=True)
        root = jnp.sqrt(n + squash_eps)
        return n, root, root / (1.0 + n)

    def squash_back(s, dc):
        n, root, fac = squash(s)
        slope = (0.5 * (1.0 + n) / root - root) / ((1.0 + n) * (1.0 + n))
        inner = jnp.sum(dc * s, axis=0, keepdims=True)
        return dc * fac + s * (2.0 * slope * inner)

    slot_acc[...] = jnp.zeros_like(slot_acc)
    pos_iota = lax.broadcasted_iota(jnp.int32, (padded, lanes), 0)

    def per_block(b, carry):
        live = pos_iota < lens_ref[pl.ds(b, 1), :]

        def softmax(v):
            e = jnp.exp(v)
            return e / over_interests(e)

        def keep_vec(vec_t, j):
            vb = vec_t.astype(bf16)
            vcat[j * lanes:(j + 1) * lanes, :] = vb.T
            return vb

        logit1 = logit_ref[b]
        p1 = softmax(logit1)
        spread(jnp.where(live, p1, 0.0), 0)
        s1 = by_interest(bilt_ref, weighted_sum(b, 0))
        c1 = s1 * squash(s1)[2]
        u1 = keep_vec(by_interest(bil_ref, c1), 3)
        logit2 = logit1 + agreement(b, u1)
        p2 = softmax(logit2)
        spread(jnp.where(live, p2, 0.0), 1)
        s2 = by_interest(bilt_ref, weighted_sum(b, 1))
        c2 = s2 * squash(s2)[2]
        u2 = keep_vec(by_interest(bil_ref, c2), 4)
        logit3 = logit2 + agreement(b, u2)
        p3 = softmax(logit3)
        spread(jnp.where(live, p3, 0.0), 2)
        s3 = by_interest(bilt_ref, weighted_sum(b, 2))
        c3 = s3 * squash(s3)[2]
        interests_ref[b] = c3.astype(bf16).T
        ds3 = squash_back(s3, cot_ref[b])
        v3 = keep_vec(by_interest(bil_ref, ds3), 2)
        dp3 = jnp.where(live, agreement(b, v3), 0.0)
        dl3 = p3 * (dp3 - over_interests(p3 * dp3))
        spread(dl3, 4)
        dc2 = by_interest(bilt_ref, weighted_sum(b, 4))
        ds2 = squash_back(s2, dc2)
        v2 = keep_vec(by_interest(bil_ref, ds2), 1)
        dp2 = jnp.where(live, agreement(b, v2), 0.0)
        dl2 = dl3 + p2 * (dp2 - over_interests(p2 * dp2))
        spread(dl2, 3)
        dc1 = by_interest(bilt_ref, weighted_sum(b, 3))
        ds1 = squash_back(s1, dc1)
        keep_vec(by_interest(bil_ref, ds1), 0)
        for t in range(tile_count):
            rg_ref[t * lanes:(t + 1) * lanes, :] = dot(mcat[t * lanes:(t + 1) * lanes, :], vcat[...]).astype(bf16)

        def slot_chunk(i, carry):
            for t in range(tile_count):
                tile = b * tile_count + t
                lo3 = lo_ref[tile].reshape(cap // 16, 16, lanes)
                orow16 = jnp.broadcast_to(owner_ref[pl.ds(tile, 1), :], (16, lanes))
                for oo in range(256 // cap):
                    ind = indicator(orow16, i * (256 // cap) + oo)
                    oh_rows[oo * cap:(oo + 1) * cap, t * lanes:(t + 1) * lanes] = (
                        lo3 * ind[None]).reshape(cap, lanes)
            start = pl.multiple_of(i * 256, 256)
            slot_acc[pl.ds(start, 256), :] += dot(oh_rows[...], rg_ref[...])
            return carry

        lax.fori_loop(0, slots // 256, slot_chunk, 0)
        return carry

    lax.fori_loop(0, block_count, per_block, 0)
    slotgrad_ref[...] = slot_acc[...].astype(bf16)


def route(fetched, bilinear, history, lengths, init_logits, interest_grad, cap):
    slots, width = fetched.shape
    users, hist_count = history.shape
    interests = init_logits.shape[2]
    blocks = users // BLOCK_USERS
    tile_count = -(-hist_count // TILE_POSITIONS)
    positions = tile_count * TILE_POSITIONS
    padded = -(-positions // 8) * 8
    lanes = interests * BLOCK_USERS
    hist_t = jnp.pad(history.T, ((0, positions - hist_count), (0, 0)))
    hist_t = hist_t.reshape(tile_count, TILE_POSITIONS, blocks, BLOCK_USERS).transpose(2, 0, 1, 3)
    hist_t = hist_t.reshape(blocks * tile_count, lanes)
    owner = hist_t // cap
    slot = hist_t % cap
    lens = jnp.broadcast_to(lengths.reshape(blocks, 1, BLOCK_USERS), (blocks, interests, BLOCK_USERS)).reshape(blocks, lanes)
    logits = init_logits.reshape(blocks, BLOCK_USERS, hist_count, interests).transpose(0, 2, 3, 1)
    logits = jnp.pad(logits.reshape(blocks, hist_count, lanes), ((0, 0), (0, padded - hist_count), (0, 0)))
    cot = interest_grad.reshape(blocks, BLOCK_USERS, interests, width).transpose(0, 3, 2, 1).reshape(blocks, width, lanes)
    bilt = bilinear.reshape(width, interests, width).transpose(2, 1, 0).reshape(width, interests * width)
    vmem = functools.partial(pltpu.VMEM)
    tiles = blocks * tile_count
    rows = tile_count * lanes
    out, slot_grads = pl.pallas_call(
        functools.partial(routing_kernel, interests, tile_count),
        out_shape=(
            jax.ShapeDtypeStruct((blocks, lanes, width), bf16),
            jax.ShapeDtypeStruct((slots, width), bf16),
        ),
        scratch_shapes=[
            pltpu.VMEM((width, slots), bf16),
            pltpu.VMEM((tiles, lanes, width), bf16),
            pltpu.VMEM((tiles, width, lanes), bf16),
            pltpu.VMEM((tiles, cap, lanes), bf16),
            pltpu.VMEM((slots, lanes), bf16),
            pltpu.VMEM((slots, lanes), bf16),
            pltpu.VMEM((rows, 5 * lanes), bf16),
            pltpu.VMEM((5 * lanes, width), bf16),
            pltpu.VMEM((interests * width, lanes), bf16),
            pltpu.VMEM((rows, width), bf16),
            pltpu.VMEM((256, rows), bf16),
            pltpu.VMEM((padded, lanes), f32),
            pltpu.VMEM((slots, width), f32),
        ],
        compiler_params=pltpu.CompilerParams(vmem_limit_bytes=60 * 1024 * 1024),
    )(fetched, bilinear, bilt, owner, slot, lens, logits, cot)
    capsules = out.reshape(blocks, interests, BLOCK_USERS, width).transpose(0, 2, 1, 3).reshape(users, interests, width)
    return capsules, slot_grads


def table_kernel(target_ref, rows_ref, out_ref, rows32, acc, sem):
    count = rows_ref.shape[0]
    table_rows = out_ref.shape[0]
    rows32[...] = rows_ref[...].astype(f32)
    acc[...] = jnp.zeros_like(acc)

    def step(i, carry):
        base = pl.multiple_of(i * 8, 8)
        where = [target_ref[base + j] for j in range(8)]
        sums = [acc[pl.ds(where[j], 1), :] + rows32[pl.ds(base + j, 1), :] for j in range(8)]
        for j in range(8):
            acc[pl.ds(where[j], 1), :] = sums[j]
        return carry

    lax.fori_loop(0, count // 8, step, 0)
    copy = pltpu.make_async_copy(acc.at[pl.ds(0, table_rows), :], out_ref, sem)
    copy.start()
    copy.wait()


def add_to_table(returned, wanted, table_rows):
    count, width = returned.shape
    spare = table_rows + lax.rem(lax.broadcasted_iota(jnp.int32, (count,), 0), 8)
    targets = jnp.where(wanted >= 0, wanted, spare)
    return pl.pallas_call(
        table_kernel,
        out_shape=jax.ShapeDtypeStruct((table_rows, width), f32),
        in_specs=[
            pl.BlockSpec(memory_space=pltpu.SMEM),
            pl.BlockSpec(memory_space=pltpu.VMEM),
        ],
        out_specs=pl.BlockSpec(memory_space=pl.ANY),
        scratch_shapes=[
            pltpu.VMEM((count, width), f32),
            pltpu.VMEM((table_rows + 8, width), f32),
            pltpu.SemaphoreType.DMA,
        ],
        compiler_params=pltpu.CompilerParams(vmem_limit_bytes=60 * 1024 * 1024),
    )(targets, returned)


def exchange(x):
    return lax.all_to_all(x, AXES, split_axis=0, concat_axis=0, tiled=True)


def local(item_table, bilinear, requests, history, lengths, init_logits, interest_grad):
    asked_ids = requests[0]
    owner_count, slot_count = asked_ids.shape
    local_table_rows, width = item_table.shape
    wanted = exchange(asked_ids)
    found = item_table.at[jnp.maximum(wanted, 0).reshape(-1)].get(mode="promise_in_bounds")
    fetched = exchange(found.reshape(owner_count, slot_count, width)).reshape(owner_count * slot_count, width)
    capsules, slot_grads = route(fetched, bilinear, history, lengths, init_logits, interest_grad, slot_count)
    returned = exchange(slot_grads.reshape(owner_count, slot_count, width)).reshape(owner_count * slot_count, width)
    table_grad = add_to_table(returned, wanted.reshape(-1), local_table_rows)
    return capsules, table_grad


def solution(mesh):
    placed = (
        P(AXES, None),
        P(),
        P(AXES, None, None),
        P(AXES, None),
        P(AXES),
        P(AXES, None, None),
        P(AXES, None, None),
    )
    return jax.shard_map(
        local,
        mesh=mesh,
        in_specs=placed,
        out_specs=(P(AXES, None, None), P(AXES, None)),
        check_vma=False,
    )
```

```python
import functools

import jax
import jax.numpy as jnp
from jax import lax
from jax.experimental import pallas as pl
from jax.experimental.pallas import tpu as pltpu
from jax.sharding import PartitionSpec as P

ITERS = 3
squash_eps = 1e-06
AXES = ("gx", "gy")
BLOCK_USERS = 64
TILE_POSITIONS = 4
GROUP_USERS = 16
GROUP_ROWS = 8
COPIES = 8
VARIANTS = (8,)
f32 = jnp.float32
bf16 = jnp.bfloat16


def dot(a, b):
    return jnp.dot(a, b, preferred_element_type=f32)


def routing_kernel(
    interest_count, variants,
    need_ref, fetched_ref, bil_ref, bilt_ref, owner_ref, slot_ref, lens_ref, logit_ref, cot_ref,
    interests_ref, slotgrad_ref,
    fetched_t, gram, x_ref, xt_ref, lo_ref, oht_a, oht_b, mix, vcat, stack, rg_ref, oh_rows,
    rows_a, coefs, coef_rows, mix_g, z_ref, slot_acc,
):
    slots, width = fetched_ref.shape
    blocks, tiles, lanes = owner_ref.shape
    cap = lo_ref.shape[1]
    owners = slots // cap
    users = lanes // interest_count
    groups = users // GROUP_USERS
    group_lanes = lanes // groups
    chunk = oh_rows.shape[0]
    padded = logit_ref.shape[1]

    for c in range(0, slots, 256):
        fetched_t[:, c:c + 256] = fetched_ref[c:c + 256, :].T
    for k in range(interest_count):
        part = bil_ref[:, k * width:(k + 1) * width]
        gram[:, k * width:(k + 1) * width] = lax.dot_general(
            part, part, (((1,), (1,)), ((), ())), preferred_element_type=f32).astype(bf16)
    slot_acc[...] = jnp.zeros_like(slot_acc)
    vcat[...] = jnp.zeros_like(vcat)

    slot_iota = lax.broadcasted_iota(jnp.int32, (cap, lanes), 0)

    def col_user(lane):
        return (lane // group_lanes) * GROUP_USERS + lane % GROUP_USERS

    diag = col_user(lax.broadcasted_iota(jnp.int32, (users, lanes), 1)) == lax.broadcasted_iota(jnp.int32, (users, lanes), 0)
    lane_k = (lax.broadcasted_iota(jnp.int32, (width, lanes), 1) // GROUP_USERS) % interest_count
    half_lane = lax.broadcasted_iota(jnp.int32, (padded, 128), 1)
    mix_lanes = mix_g.shape[1]
    diag_g = (lax.broadcasted_iota(jnp.int32, (GROUP_USERS, mix_lanes), 1) % GROUP_USERS
              == lax.broadcasted_iota(jnp.int32, (GROUP_USERS, mix_lanes), 0))
    pos_iota = lax.broadcasted_iota(jnp.int32, (padded, lanes), 0)

    def indicator(orow16, o):
        return jnp.where(orow16 == o, 1.0, 0.0).astype(bf16)

    def over_interests(v):
        parts = []
        for h in range(0, lanes, 128):
            s = v[:, h:h + 128]
            step = group_lanes // 2
            while step >= GROUP_USERS:
                low = half_lane % (2 * step) < step
                s = s + jnp.where(low, pltpu.roll(s, 128 - step, 1), pltpu.roll(s, step, 1))
                step //= 2
            parts.append(s)
        return jnp.concatenate(parts, axis=1)

    def softmax(v):
        e = jnp.exp(v)
        return e / over_interests(e)

    def by_interest(mat_ref, v):
        zero = jnp.zeros_like(v)
        for k in range(interest_count):
            stack[k * width:(k + 1) * width, :] = jnp.where(lane_k == k, v, zero).astype(bf16)
        return dot(mat_ref[...], stack[...])

    def squash_parts(n):
        root = jnp.sqrt(n + squash_eps)
        fac = root / (1.0 + n)
        slope = (0.5 * (1.0 + n) / root - root) / ((1.0 + n) * (1.0 + n))
        return fac, 2.0 * slope

    def keep_vec(vec_t, j):
        vb = vec_t.astype(bf16)
        vn = vb.T
        for g in range(groups):
            vcat[g, j * group_lanes:(j + 1) * group_lanes, :] = vn[g * group_lanes:(g + 1) * group_lanes, :]
        return vb

    def block_body(b, tile_count):
        positions = tile_count * TILE_POSITIONS

        def build(t, buf):
            crow = slot_ref[b, pl.ds(t, 1), :]
            orow16 = jnp.broadcast_to(owner_ref[b, pl.ds(t, 1), :], (16, lanes))
            lo = jnp.where(slot_iota == crow, 1.0, 0.0).astype(bf16)
            lo_ref[t] = lo
            lo3 = lo.reshape(cap // 16, 16, lanes)
            for o in range(owners):
                buf[o * cap:(o + 1) * cap, :] = (lo3 * indicator(orow16, o)[None]).reshape(cap, lanes)

        def gather(t, buf):
            xtb = dot(fetched_t[...], buf[...]).astype(bf16)
            xt_ref[t] = xtb
            x_ref[t] = xtb.T

        build(0, oht_a)

        def gather_pair(i, carry):
            t = 2 * i
            build(t + 1, oht_b)
            gather(t, oht_a)
            build(jnp.minimum(t + 2, tile_count - 1), oht_a)
            gather(t + 1, oht_b)
            return carry

        lax.fori_loop(0, tile_count // 2, gather_pair, 0)
        if tile_count % 2:
            gather(tile_count - 1, oht_a)

        def weighted_sum(coef, j):
            coefs[j] = coef
            for l in range(positions):
                row = jnp.broadcast_to(coefs[j, l:l + 1, :], (users, lanes))
                mix[l * users:(l + 1) * users, :] = jnp.where(diag, row, 0.0).astype(bf16)
            total = jnp.zeros((width, lanes), f32)
            for t in range(tile_count):
                total = total + dot(xt_ref[t], mix[t * lanes:(t + 1) * lanes, :])
            return total

        def agreement(vec):
            for t in range(tile_count):
                prod = dot(x_ref[t], vec)
                for p in range(TILE_POSITIONS):
                    part = jnp.where(diag, prod[p * users:(p + 1) * users, :], 0.0)
                    l = t * TILE_POSITIONS + p
                    rows_a[l:l + 1, :] = jnp.sum(part, axis=0, keepdims=True)
            return jnp.where(live, rows_a[...], 0.0)

        live = pos_iota < lens_ref[pl.ds(b, 1), :]
        zero = jnp.zeros((padded, lanes), f32)

        def turn(p, j):
            xs = weighted_sum(jnp.where(live, p, zero), j)
            z = by_interest(gram, xs)
            n = jnp.maximum(jnp.sum(xs * z, axis=0, keepdims=True), 0.0)
            fac, slope = squash_parts(n)
            z_ref[j] = z
            return fac, slope, keep_vec(z * fac, 3 + j)

        logit1 = logit_ref[b]
        p1 = softmax(logit1)
        fac1, slope1, u1 = turn(p1, 0)
        logit2 = logit1 + agreement(u1)
        p2 = softmax(logit2)
        fac2, slope2, u2 = turn(p2, 1)
        logit3 = logit2 + agreement(u2)
        p3 = softmax(logit3)
        s3 = by_interest(bilt_ref, weighted_sum(jnp.where(live, p3, zero), 2))
        fac3, slope3 = squash_parts(jnp.sum(s3 * s3, axis=0, keepdims=True))
        interests_ref[b] = (s3 * fac3).astype(bf16).T
        dc3 = cot_ref[b]
        ds3 = dc3 * fac3 + s3 * (slope3 * jnp.sum(dc3 * s3, axis=0, keepdims=True))
        v3 = keep_vec(by_interest(bil_ref, ds3), 2)

        def turn_back(p, dp, later, j_vec, j_coef, fac, slope):
            dl = jnp.where(live, later + p * (dp - over_interests(p * dp)), zero)
            dxs = weighted_sum(dl, j_coef)
            y = by_interest(gram, dxs)
            z = z_ref[j_vec]
            inner = slope * jnp.sum(dxs * z, axis=0, keepdims=True)
            return dl, keep_vec(y * fac + z * inner, j_vec)

        dl3, v2 = turn_back(p3, agreement(v3), zero, 1, 4, fac2, slope2)
        turn_back(p2, agreement(v2), dl3, 0, 3, fac1, slope1)

        for g in range(groups):
            src = (g * group_lanes) // 128 * 128
            odd = (g * group_lanes) % 128

            def piece(j, dest):
                x = coefs[j, :, src:src + 128]
                return x if odd == dest else pltpu.roll(x, 64, 1)

            for q in range(0, 5, 2):
                low = piece(q, 0)
                high = piece(q + 1, 64) if q + 1 < 5 else jnp.zeros((padded, 128), f32)
                coef_rows[:, q * 64:q * 64 + 128] = jnp.where(half_lane < 64, low, high)
            for l in range(positions):
                row = jnp.broadcast_to(coef_rows[l:l + 1, :], (GROUP_USERS, mix_lanes))
                mix_g[l * GROUP_USERS:(l + 1) * GROUP_USERS, :] = jnp.where(diag_g, row, 0.0).astype(bf16)
            grads = dot(mix_g[0:positions * GROUP_USERS, :], vcat[g]).astype(bf16)
            for l in range(positions):
                start = l * users + g * GROUP_USERS
                rg_ref[start:start + GROUP_USERS, :] = grads[l * GROUP_USERS:(l + 1) * GROUP_USERS, :]

        def slot_chunk(i, carry):
            for t in range(tile_count):
                lo3 = lo_ref[t].reshape(cap // 16, 16, lanes)
                orow16 = jnp.broadcast_to(owner_ref[b, t:t + 1, :], (16, lanes))
                for oo in range(chunk // cap):
                    ind = indicator(orow16, i * (chunk // cap) + oo)
                    oh_rows[oo * cap:(oo + 1) * cap, t * lanes:(t + 1) * lanes] = (
                        lo3 * ind[None]).reshape(cap, lanes)
            start = pl.multiple_of(i * chunk, chunk)
            rows = tile_count * lanes
            slot_acc[pl.ds(start, chunk), :] += dot(oh_rows[:, 0:rows], rg_ref[0:rows, :])
            return carry

        lax.fori_loop(0, slots // chunk, slot_chunk, 0)

    def per_block(b, carry):
        need = need_ref[b]
        for i, count in enumerate(variants):
            fits = need <= count
            if i + 1 < len(variants):
                fits = jnp.logical_and(fits, need > variants[i + 1])

            @pl.when(fits)
            def _():
                block_body(b, count)

        return carry

    lax.fori_loop(0, blocks, per_block, 0)
    slotgrad_ref[...] = slot_acc[...].astype(bf16)


def prepare(history, lengths, init_logits, interest_grad, cap):
    users, hist_count = history.shape
    interests = init_logits.shape[2]
    width = interest_grad.shape[2]
    lanes = interests * BLOCK_USERS
    blocks = users // BLOCK_USERS
    tile_count = -(-hist_count // TILE_POSITIONS)
    positions = tile_count * TILE_POSITIONS
    padded = -(-positions // 8) * 8
    index = lax.iota(jnp.int32, users)
    ahead = (lengths[None, :] > lengths[:, None]) | (
        (lengths[None, :] == lengths[:, None]) & (index[None, :] < index[:, None]))
    rank = jnp.sum(ahead.astype(jnp.int32), axis=1)
    order = (rank[:, None] == index[None, :]).astype(bf16)
    column = lax.iota(jnp.int32, users * interests)
    block, rest = column // lanes, column % lanes
    group_lanes = interests * GROUP_USERS
    user = block * BLOCK_USERS + rest // group_lanes * GROUP_USERS + rest % GROUP_USERS
    interest = rest // GROUP_USERS % interests
    select = ((rank[:, None, None] == user[None, None, :])
              & (lax.iota(jnp.int32, interests)[None, :, None] == interest[None, None, :]))
    select = select.reshape(users * interests, users * interests)
    by_k = ((rank[None, :, None] == user[None, None, :])
            & (lax.iota(jnp.int32, interests)[:, None, None] == interest[None, None, :]))
    by_k = by_k.reshape(users * interests, users * interests)

    def sort_positions(values):
        s = jnp.dot(values.astype(bf16).T, order, preferred_element_type=f32).astype(jnp.int32)
        s = jnp.pad(s, ((0, positions - hist_count), (0, 0)))
        s = s.reshape(tile_count, TILE_POSITIONS, blocks, BLOCK_USERS).transpose(2, 0, 1, 3)
        return s.reshape(blocks, tile_count, TILE_POSITIONS * BLOCK_USERS)

    owner = sort_positions(history // cap)
    slot = sort_positions(history % cap)
    sorted_lens = jnp.sum(jnp.where(rank[:, None] == index[None, :], lengths[:, None], 0), axis=0)
    need = (sorted_lens[::BLOCK_USERS] + TILE_POSITIONS - 1) // TILE_POSITIONS
    lens = jnp.sum(jnp.where(rank[:, None] == user[None, :], lengths[:, None], 0), axis=0).reshape(blocks, lanes)
    flat = init_logits.transpose(1, 2, 0).reshape(hist_count, interests * users)
    logits = jnp.dot(flat, by_k.astype(f32), precision=lax.Precision.HIGHEST, preferred_element_type=f32)
    logits = jnp.pad(logits, ((0, padded - hist_count), (0, 0))).reshape(padded, blocks, lanes).transpose(1, 0, 2)
    grads = interest_grad.reshape(users * interests, width)
    cot = lax.dot_general(grads.astype(bf16), select.astype(bf16), (((0,), (0,)), ((), ())), preferred_element_type=f32)
    cot = cot.reshape(width, blocks, lanes).transpose(1, 0, 2)
    return owner, slot, need, lens, logits, cot, select


def route(fetched, bilinear, prepared, cap):
    owner, slot, need, lens, logits, cot, select = prepared
    slots, width = fetched.shape
    blocks, tile_count, lanes = owner.shape
    padded = logits.shape[1]
    interests = bilinear.shape[1] // width
    users = lanes // interests
    groups = users // GROUP_USERS
    mix_lanes = -(-5 * lanes // groups // 128) * 128
    bilt = bilinear.reshape(width, interests, width).transpose(2, 1, 0).reshape(width, interests * width)
    rows = tile_count * lanes
    variants = [tile_count] + [v for v in VARIANTS if v < tile_count]
    chunk = 512
    out, slot_grads = pl.pallas_call(
        functools.partial(routing_kernel, interests, variants),
        out_shape=(
            jax.ShapeDtypeStruct((blocks, lanes, width), bf16),
            jax.ShapeDtypeStruct((slots, width), bf16),
        ),
        in_specs=[pl.BlockSpec(memory_space=pltpu.SMEM)] + [pl.BlockSpec(memory_space=pltpu.VMEM)] * 8,
        scratch_shapes=[
            pltpu.VMEM((width, slots), bf16),
            pltpu.VMEM((width, interests * width), bf16),
            pltpu.VMEM((tile_count, lanes, width), bf16),
            pltpu.VMEM((tile_count, width, lanes), bf16),
            pltpu.VMEM((tile_count, cap, lanes), bf16),
            pltpu.VMEM((slots, lanes), bf16),
            pltpu.VMEM((slots, lanes), bf16),
            pltpu.VMEM((rows, lanes), bf16),
            pltpu.VMEM((groups, mix_lanes, width), bf16),
            pltpu.VMEM((interests * width, lanes), bf16),
            pltpu.VMEM((rows, width), bf16),
            pltpu.VMEM((chunk, rows), bf16),
            pltpu.VMEM((padded, lanes), f32),
            pltpu.VMEM((5, padded, lanes), f32),
            pltpu.VMEM((padded, mix_lanes), f32),
            pltpu.VMEM((rows // groups, mix_lanes), bf16),
            pltpu.VMEM((2, width, lanes), f32),
            pltpu.VMEM((slots, width), f32),
        ],
        compiler_params=pltpu.CompilerParams(vmem_limit_bytes=60 * 1024 * 1024),
    )(need, fetched, bilinear, bilt, owner, slot, lens, logits, cot)
    capsules = jnp.dot(select.astype(bf16), out.reshape(blocks * lanes, width), preferred_element_type=f32)
    return capsules.astype(bf16).reshape(blocks * users, interests, width), slot_grads


def fetch_kernel(wanted_ref, table_ref, out_ref, staged, table32, rows32, sems):
    parts = sems.shape[0]
    part = table_ref.shape[0] // parts
    copies = [
        pltpu.make_async_copy(table_ref.at[pl.ds(p * part, part), :], staged.at[pl.ds(p * part, part), :], sems.at[p])
        for p in range(parts)
    ]
    for copy in copies:
        copy.start()
    for p in range(parts):
        copies[p].wait()

        def widen(i, carry):
            base = pl.multiple_of(p * part + i * 128, 128)
            table32[pl.ds(base, 128), :] = staged[pl.ds(base, 128), :].astype(f32)
            return carry

        lax.fori_loop(0, part // 128, widen, 0)

    def copy_rows(i, carry):
        base = pl.multiple_of(i * 8, 8)
        rows = [table32[pl.ds(wanted_ref[base + j], 1), :] for j in range(8)]
        rows32[pl.ds(base, 8), :] = jnp.concatenate(rows, axis=0)
        return carry

    lax.fori_loop(0, out_ref.shape[0] // 8, copy_rows, 0, unroll=2)
    out_ref[...] = rows32[...].astype(bf16)


def fetch_rows(table, wanted):
    table_rows, width = table.shape
    count = wanted.shape[0]
    return pl.pallas_call(
        fetch_kernel,
        out_shape=jax.ShapeDtypeStruct((count, width), bf16),
        in_specs=[pl.BlockSpec(memory_space=pltpu.SMEM), pl.BlockSpec(memory_space=pl.ANY)],
        scratch_shapes=[
            pltpu.VMEM((table_rows, width), bf16),
            pltpu.VMEM((table_rows, width), f32),
            pltpu.VMEM((count, width), f32),
            pltpu.SemaphoreType.DMA((COPIES,)),
        ],
        compiler_params=pltpu.CompilerParams(vmem_limit_bytes=60 * 1024 * 1024),
    )(wanted, table)


def table_kernel(target_ref, rows_ref, out_ref, acc, sems):
    count = rows_ref.shape[0]
    parts = sems.shape[0]
    part = out_ref.shape[0] // parts
    acc[...] = jnp.zeros_like(acc)

    def step(i, carry):
        base = pl.multiple_of(i * 16, 16)
        rows = rows_ref[pl.ds(base, 16), :].astype(f32)
        where = [target_ref[base + j] for j in range(16)]
        for q in range(0, 16, GROUP_ROWS):
            sums = [acc[pl.ds(where[j], 1), :] + rows[j:j + 1, :] for j in range(q, q + GROUP_ROWS)]
            for j in range(q, q + GROUP_ROWS):
                acc[pl.ds(where[j], 1), :] = sums[j - q]
        return carry

    lax.fori_loop(0, count // 16, step, 0, unroll=2)
    copies = [
        pltpu.make_async_copy(acc.at[pl.ds(p * part, part), :], out_ref.at[pl.ds(p * part, part), :], sems.at[p])
        for p in range(parts)
    ]
    for copy in copies:
        copy.start()
    for copy in copies:
        copy.wait()


def add_to_table(returned, wanted, table_rows):
    count, width = returned.shape
    spare = table_rows + lax.rem(lax.broadcasted_iota(jnp.int32, (count,), 0), GROUP_ROWS)
    targets = jnp.where(wanted >= 0, wanted, spare)
    return pl.pallas_call(
        table_kernel,
        out_shape=jax.ShapeDtypeStruct((table_rows, width), f32),
        in_specs=[pl.BlockSpec(memory_space=pltpu.SMEM), pl.BlockSpec(memory_space=pltpu.VMEM)],
        out_specs=pl.BlockSpec(memory_space=pl.ANY),
        scratch_shapes=[
            pltpu.VMEM((table_rows + GROUP_ROWS, width), f32),
            pltpu.SemaphoreType.DMA((COPIES,)),
        ],
        compiler_params=pltpu.CompilerParams(vmem_limit_bytes=60 * 1024 * 1024),
    )(targets, returned)


def exchange(x):
    return lax.all_to_all(x, AXES, split_axis=0, concat_axis=0, tiled=True)


def local(item_table, bilinear, requests, history, lengths, init_logits, interest_grad):
    asked_ids = requests[0]
    owner_count, slot_count = asked_ids.shape
    local_table_rows, width = item_table.shape
    wanted = exchange(asked_ids)
    found = fetch_rows(item_table, jnp.maximum(wanted, 0).reshape(-1))
    fetched = exchange(found.reshape(owner_count, slot_count, width)).reshape(owner_count * slot_count, width)
    prepared = prepare(history, lengths, init_logits, interest_grad, slot_count)
    capsules, slot_grads = route(fetched, bilinear, prepared, slot_count)
    returned = exchange(slot_grads.reshape(owner_count, slot_count, width)).reshape(owner_count * slot_count, width)
    table_grad = add_to_table(returned, wanted.reshape(-1), local_table_rows)
    return capsules, table_grad


def solution(mesh):
    placed = (
        P(AXES, None),
        P(),
        P(AXES, None, None),
        P(AXES, None),
        P(AXES),
        P(AXES, None, None),
        P(AXES, None, None),
    )
    return jax.shard_map(
        local,
        mesh=mesh,
        in_specs=placed,
        out_specs=(P(AXES, None, None), P(AXES, None)),
        check_vma=False,
    )
```

```python
import functools

import jax
import jax.numpy as jnp
from jax import lax
from jax.experimental import pallas as pl
from jax.experimental.pallas import tpu as pltpu
from jax.sharding import PartitionSpec as P

ITERS = 3
squash_eps = 1e-06
AXES = ("gx", "gy")
BLOCK_USERS = 64
TILE_POSITIONS = 4
GROUP_USERS = 16
GROUP_ROWS = 8
COPIES = 8
OCTET = 8
PAIRS = 7
VMEM_BYTES = 60 * 1024 * 1024
f32 = jnp.float32
bf16 = jnp.bfloat16


def dot(a, b):
    return jnp.dot(a, b, preferred_element_type=f32)


def routing_kernel(
    interest_count,
    meta_ref, fetched_ref, bil_ref, bilt_ref, owner_ref, slot_ref, lens_ref, logit_ref, cot_ref,
    interests_ref, slotgrad_ref,
    fetched_t, gram, x_ref, xt_ref, lo_ref, oht_a, oht_b, mix, vecs, vcat, stack, oh_rows,
    sums, logit_now, p_ref, coefs, mix_g, z_ref, slot_acc,
):
    slots, width = fetched_ref.shape
    lanes = owner_ref.shape[2]
    blocks = interests_ref.shape[0]
    pair_max = xt_ref.shape[0]
    pair_rows = xt_ref.shape[2]
    cap = lo_ref.shape[1]
    owners = slots // cap
    users = lanes // interest_count
    groups = users // GROUP_USERS
    group_lanes = lanes // groups
    chunk = oh_rows.shape[0]
    mix_lanes = mix_g.shape[2]
    chunk_count = meta_ref[2 * pair_max]

    for c in range(0, slots, 256):
        fetched_t[:, c:c + 256] = fetched_ref[c:c + 256, :].T
    for k in range(interest_count):
        part = bil_ref[:, k * width:(k + 1) * width]
        gram[:, k * width:(k + 1) * width] = lax.dot_general(
            part, part, (((1,), (1,)), ((), ())), preferred_element_type=f32).astype(bf16)
    slot_acc[...] = jnp.zeros_like(slot_acc)
    vcat[...] = jnp.zeros_like(vcat)
    vecs[...] = jnp.zeros_like(vecs)

    slot_iota = lax.broadcasted_iota(jnp.int32, (cap, lanes), 0)

    def col_user(lane):
        return (lane // group_lanes) * GROUP_USERS + lane % GROUP_USERS

    diag = col_user(lax.broadcasted_iota(jnp.int32, (users, lanes), 1)) == lax.broadcasted_iota(jnp.int32, (users, lanes), 0)
    lane_k = (lax.broadcasted_iota(jnp.int32, (width, lanes), 1) // GROUP_USERS) % interest_count
    half_lane = lax.broadcasted_iota(jnp.int32, (OCTET, 128), 1)
    diag_g = (lax.broadcasted_iota(jnp.int32, (GROUP_USERS, mix_lanes), 1) % GROUP_USERS
              == lax.broadcasted_iota(jnp.int32, (GROUP_USERS, mix_lanes), 0))
    pos_iota = lax.broadcasted_iota(jnp.int32, (OCTET, lanes), 0)

    def place(i):
        return meta_ref[i], meta_ref[pair_max + i]

    def flat(i):
        return pl.ds(pl.multiple_of(i * OCTET, OCTET), OCTET)

    def pair_at(i):
        return pl.ds(pl.multiple_of(i * pair_rows, pair_rows), pair_rows)

    def indicator(orow16, o):
        return jnp.where(orow16 == o, 1.0, 0.0).astype(bf16)

    def over_interests(v):
        parts = []
        for h in range(0, lanes, 128):
            s = v[:, h:h + 128]
            step = group_lanes // 2
            while step >= GROUP_USERS:
                low = half_lane % (2 * step) < step
                s = s + jnp.where(low, pltpu.roll(s, 128 - step, 1), pltpu.roll(s, step, 1))
                step //= 2
            parts.append(s)
        return jnp.concatenate(parts, axis=1)

    def softmax(v):
        e = jnp.exp(v)
        return e / over_interests(e)

    def by_interest(b, mat_ref, v):
        zero = jnp.zeros_like(v)
        for k in range(interest_count):
            stack[b, k * width:(k + 1) * width, :] = jnp.where(lane_k == k, v, zero).astype(bf16)
        return dot(mat_ref[...], stack[b])

    def squash_parts(n):
        root = jnp.sqrt(n + squash_eps)
        fac = root / (1.0 + n)
        slope = (0.5 * (1.0 + n) / root - root) / ((1.0 + n) * (1.0 + n))
        return fac, 2.0 * slope

    def keep_vec(b, vec_t, j):
        vb = vec_t.astype(bf16)
        vecs[b] = vb
        vn = vb.T
        for g in range(groups):
            vcat[b, g, j * group_lanes:(j + 1) * group_lanes, :] = vn[g * group_lanes:(g + 1) * group_lanes, :]

    def build(i, j, buf):
        b, o8 = place(i)
        row = 2 * o8 + j
        crow = slot_ref[b, pl.ds(row, 1), :]
        orow16 = jnp.broadcast_to(owner_ref[b, pl.ds(row, 1), :], (16, lanes))
        lo = jnp.where(slot_iota == crow, 1.0, 0.0).astype(bf16)
        lo_ref[2 * i + j] = lo
        lo3 = lo.reshape(cap // 16, 16, lanes)
        for o in range(owners):
            buf[o * cap:(o + 1) * cap, :] = (lo3 * indicator(orow16, o)[None]).reshape(cap, lanes)

    def gather(i, j, buf):
        xtb = dot(fetched_t[...], buf[...]).astype(bf16)
        xt_ref[i, :, j * lanes:(j + 1) * lanes] = xtb
        start = pl.multiple_of(i * pair_rows + j * lanes, lanes)
        x_ref[pl.ds(start, lanes), :] = xtb.T

    pairs = chunk_count * PAIRS
    build(0, 0, oht_a)

    def gather_pair(i, carry):
        build(i, 1, oht_b)
        gather(i, 0, oht_a)
        build(jnp.minimum(i + 1, pairs - 1), 0, oht_a)
        gather(i, 1, oht_b)
        return carry

    lax.fori_loop(0, pairs, gather_pair, 0)

    def over_pairs(body):
        sums[...] = jnp.zeros_like(sums)

        def step(c, carry):
            work = []
            for q in range(PAIRS):
                i = c * PAIRS + q
                b, o8 = place(i)
                live = pos_iota + o8 * OCTET < lens_ref[pl.ds(b, 1), :]
                work.append((i, b, o8, live))
            coef = body(work)
            for q, (i, b, o8, live) in enumerate(work):
                for l in range(OCTET):
                    row = jnp.broadcast_to(coef[q][l:l + 1, :], (users, lanes))
                    mix[q, l * users:(l + 1) * users, :] = jnp.where(diag, row, 0.0).astype(bf16)
            for q, (i, b, o8, live) in enumerate(work):
                sums[b] += dot(xt_ref[i], mix[q])
            return carry

        lax.fori_loop(0, chunk_count, step, 0)

    def agreement(i, b, live):
        rows = []
        prod = dot(x_ref[pair_at(i), :], vecs[b])
        for l in range(OCTET):
            part = jnp.where(diag, prod[l * users:(l + 1) * users, :], 0.0)
            rows.append(jnp.sum(part, axis=0, keepdims=True))
        return jnp.where(live, jnp.concatenate(rows, axis=0), 0.0)

    def weigh(i, live, logits, j):
        p = softmax(logits)
        if j > 0:
            p_ref[j - 1, flat(i), :] = p
        w = jnp.where(live, p, 0.0)
        coefs[j, flat(i), :] = w
        return w

    def first(work):
        out = []
        for i, b, o8, live in work:
            logits = logit_ref[b, flat(o8), :]
            logit_now[flat(i), :] = logits
            out.append(weigh(i, live, logits, 0))
        return out

    def later(j):
        def body(work):
            out = []
            agreed = [agreement(i, b, live) for i, b, o8, live in work]
            for a, (i, b, o8, live) in zip(agreed, work):
                logits = logit_now[flat(i), :] + a
                if j == 1:
                    logit_now[flat(i), :] = logits
                out.append(weigh(i, live, logits, j))
            return out
        return body

    def back(j_prob, j_coef, j_later):
        def body(work):
            out = []
            agreed = [agreement(i, b, live) for i, b, o8, live in work]
            for dp, (i, b, o8, live) in zip(agreed, work):
                p = p_ref[j_prob, flat(i), :]
                dl = p * (dp - over_interests(p * dp))
                if j_later is not None:
                    dl = dl + coefs[j_later, flat(i), :]
                dl = jnp.where(live, dl, 0.0)
                coefs[j_coef, flat(i), :] = dl
                out.append(dl)
            return out
        return body

    squashed = [None, None]

    def turn(j):
        parts = []
        for b in range(blocks):
            xs = sums[b]
            z = by_interest(b, gram, xs)
            n = jnp.maximum(jnp.sum(xs * z, axis=0, keepdims=True), 0.0)
            fac, slope = squash_parts(n)
            z_ref[j, b] = z
            keep_vec(b, z * fac, 3 + j)
            parts.append((fac, slope))
        squashed[j] = parts

    def turn_back(j):
        for b in range(blocks):
            dxs = sums[b]
            y = by_interest(b, gram, dxs)
            z = z_ref[j, b]
            fac, slope = squashed[j][b]
            inner = slope * jnp.sum(dxs * z, axis=0, keepdims=True)
            keep_vec(b, y * fac + z * inner, j)

    over_pairs(first)
    turn(0)
    over_pairs(later(1))
    turn(1)
    over_pairs(later(2))
    outs = [by_interest(b, bilt_ref, sums[b]) for b in range(blocks)]
    cots = []
    for b, s3 in enumerate(outs):
        fac3, slope3 = squash_parts(jnp.sum(s3 * s3, axis=0, keepdims=True))
        interests_ref[b] = (s3 * fac3).astype(bf16).T
        dc3 = cot_ref[b]
        cots.append(dc3 * fac3 + s3 * (slope3 * jnp.sum(dc3 * s3, axis=0, keepdims=True)))
    for b, ds3 in enumerate(cots):
        keep_vec(b, by_interest(b, bil_ref, ds3), 2)
    over_pairs(back(1, 4, None))
    turn_back(1)
    over_pairs(back(0, 3, 4))
    turn_back(0)

    def row_grads(c, carry):
        for q in range(PAIRS):
            i = c * PAIRS + q
            b, o8 = place(i)
            for g in range(groups):
                src = (g * group_lanes) // 128 * 128
                odd = (g * group_lanes) % 128

                def piece(j, dest):
                    x = coefs[j, flat(i), src:src + 128]
                    return x if odd == dest else pltpu.roll(x, 64, 1)

                parts = []
                for h in range(0, 5, 2):
                    high = piece(h + 1, 64) if h + 1 < 5 else jnp.zeros((OCTET, 128), f32)
                    parts.append(jnp.where(half_lane < 64, piece(h, 0), high))
                row8 = jnp.concatenate(parts, axis=1)
                for l in range(OCTET):
                    row = jnp.broadcast_to(row8[l:l + 1, :], (GROUP_USERS, mix_lanes))
                    mix_g[q * groups + g, l * GROUP_USERS:(l + 1) * GROUP_USERS, :] = (
                        jnp.where(diag_g, row, 0.0).astype(bf16))
        for q in range(PAIRS):
            i = c * PAIRS + q
            b, o8 = place(i)
            for g in range(groups):
                grads = dot(mix_g[q * groups + g], vcat[b, g]).astype(bf16)
                for l in range(OCTET):
                    start = pl.multiple_of(i * pair_rows + (l * users + g * GROUP_USERS), GROUP_USERS)
                    x_ref[pl.ds(start, GROUP_USERS), :] = grads[l * GROUP_USERS:(l + 1) * GROUP_USERS, :]
        return carry

    lax.fori_loop(0, chunk_count, row_grads, 0)

    def scatter(c, carry):
        def slot_chunk(s, carry):
            for q in range(PAIRS):
                i = c * PAIRS + q
                b, o8 = place(i)
                for j in range(2):
                    lo3 = lo_ref[2 * i + j].reshape(cap // 16, 16, lanes)
                    orow16 = jnp.broadcast_to(owner_ref[b, pl.ds(2 * o8 + j, 1), :], (16, lanes))
                    t = 2 * q + j
                    for oo in range(chunk // cap):
                        ind = indicator(orow16, s * (chunk // cap) + oo)
                        oh_rows[oo * cap:(oo + 1) * cap, t * lanes:(t + 1) * lanes] = (
                            lo3 * ind[None]).reshape(cap, lanes)
            start = pl.multiple_of(s * chunk, chunk)
            rows = pl.ds(pl.multiple_of(c * PAIRS * pair_rows, PAIRS * pair_rows), PAIRS * pair_rows)
            slot_acc[pl.ds(start, chunk), :] += dot(oh_rows[...], x_ref[rows, :])
            return carry

        return lax.fori_loop(0, slots // chunk, slot_chunk, carry)

    lax.fori_loop(0, chunk_count, scatter, 0)
    slotgrad_ref[...] = slot_acc[...].astype(bf16)


def prepare(history, lengths, init_logits, interest_grad, cap):
    users, hist_count = history.shape
    interests = init_logits.shape[2]
    width = interest_grad.shape[2]
    lanes = interests * BLOCK_USERS
    blocks = users // BLOCK_USERS
    octets = -(-hist_count // OCTET)
    positions = octets * OCTET
    index = lax.iota(jnp.int32, users)
    ahead = (lengths[None, :] > lengths[:, None]) | (
        (lengths[None, :] == lengths[:, None]) & (index[None, :] < index[:, None]))
    rank = jnp.sum(ahead.astype(jnp.int32), axis=1)
    order = (rank[:, None] == index[None, :]).astype(bf16)
    column = lax.iota(jnp.int32, users * interests)
    block, rest = column // lanes, column % lanes
    group_lanes = interests * GROUP_USERS
    user = block * BLOCK_USERS + rest // group_lanes * GROUP_USERS + rest % GROUP_USERS
    interest = rest // GROUP_USERS % interests
    select = ((rank[:, None, None] == user[None, None, :])
              & (lax.iota(jnp.int32, interests)[None, :, None] == interest[None, None, :]))
    select = select.reshape(users * interests, users * interests)
    by_k = ((rank[None, :, None] == user[None, None, :])
            & (lax.iota(jnp.int32, interests)[:, None, None] == interest[None, None, :]))
    by_k = by_k.reshape(users * interests, users * interests)

    def sort_positions(values):
        s = jnp.dot(values.astype(bf16).T, order, preferred_element_type=f32).astype(jnp.int32)
        s = jnp.pad(s, ((0, positions - hist_count), (0, 0)))
        s = s.reshape(positions // TILE_POSITIONS, TILE_POSITIONS, blocks, BLOCK_USERS).transpose(2, 0, 1, 3)
        s = s.reshape(blocks, positions // TILE_POSITIONS, TILE_POSITIONS * BLOCK_USERS)
        return jnp.pad(s, ((0, 1), (0, 0), (0, 0)))

    owner = sort_positions(history // cap)
    slot = sort_positions(history % cap)
    sorted_lens = jnp.sum(jnp.where(rank[:, None] == index[None, :], lengths[:, None], 0), axis=0)
    need = (sorted_lens[::BLOCK_USERS] + OCTET - 1) // OCTET
    upto = jnp.sum(jnp.where(lax.iota(jnp.int32, blocks)[None, :] <= lax.iota(jnp.int32, blocks)[:, None], need[None, :], 0), axis=1)
    pair_max = -(-blocks * octets // PAIRS) * PAIRS
    pair = lax.iota(jnp.int32, pair_max)
    passed = pair[:, None] >= upto[None, :]
    pair_block = jnp.sum(passed.astype(jnp.int32), axis=1)
    pair_octet = jnp.where(pair_block < blocks, pair - jnp.sum(jnp.where(passed, need[None, :], 0), axis=1), 0)
    chunks = (jnp.sum(need) + PAIRS - 1) // PAIRS
    meta = jnp.concatenate([pair_block, pair_octet, chunks[None]])
    lens = jnp.sum(jnp.where(rank[:, None] == user[None, :], lengths[:, None], 0), axis=0).reshape(blocks, lanes)
    lens = jnp.pad(lens, ((0, 1), (0, 0)))
    flat = init_logits.transpose(1, 2, 0).reshape(hist_count, interests * users)
    logits = jnp.dot(flat, by_k.astype(f32), precision=lax.Precision.HIGHEST, preferred_element_type=f32)
    logits = jnp.pad(logits, ((0, positions - hist_count), (0, lanes))).reshape(positions, blocks + 1, lanes).transpose(1, 0, 2)
    grads = interest_grad.reshape(users * interests, width)
    cot = lax.dot_general(grads.astype(bf16), select.astype(bf16), (((0,), (0,)), ((), ())), preferred_element_type=f32)
    cot = cot.reshape(width, blocks, lanes).transpose(1, 0, 2)
    return owner, slot, meta, lens, logits, cot, select


def route(fetched, bilinear, prepared, cap):
    owner, slot, meta, lens, logits, cot, select = prepared
    slots, width = fetched.shape
    blocks, _, lanes = cot.shape
    interests = bilinear.shape[1] // width
    users = lanes // interests
    groups = users // GROUP_USERS
    pair_max = (meta.shape[0] - 1) // 2
    pair_rows = OCTET * users
    mix_lanes = -(-5 * lanes // groups // 128) * 128
    bilt = bilinear.reshape(width, interests, width).transpose(2, 1, 0).reshape(width, interests * width)
    chunk = 512
    out, slot_grads = pl.pallas_call(
        functools.partial(routing_kernel, interests),
        out_shape=(
            jax.ShapeDtypeStruct((blocks, lanes, width), bf16),
            jax.ShapeDtypeStruct((slots, width), bf16),
        ),
        in_specs=[pl.BlockSpec(memory_space=pltpu.SMEM)] + [pl.BlockSpec(memory_space=pltpu.VMEM)] * 8,
        scratch_shapes=[
            pltpu.VMEM((width, slots), bf16),
            pltpu.VMEM((width, interests * width), bf16),
            pltpu.VMEM((pair_max * pair_rows, width), bf16),
            pltpu.VMEM((pair_max, width, pair_rows), bf16),
            pltpu.VMEM((pair_max * 2, cap, lanes), bf16),
            pltpu.VMEM((slots, lanes), bf16),
            pltpu.VMEM((slots, lanes), bf16),
            pltpu.VMEM((PAIRS, pair_rows, lanes), bf16),
            pltpu.VMEM((blocks + 1, width, lanes), bf16),
            pltpu.VMEM((blocks + 1, groups, mix_lanes, width), bf16),
            pltpu.VMEM((blocks, interests * width, lanes), bf16),
            pltpu.VMEM((chunk, PAIRS * pair_rows), bf16),
            pltpu.VMEM((blocks + 1, width, lanes), f32),
            pltpu.VMEM((pair_max * OCTET, lanes), f32),
            pltpu.VMEM((2, pair_max * OCTET, lanes), f32),
            pltpu.VMEM((5, pair_max * OCTET, lanes), f32),
            pltpu.VMEM((PAIRS * groups, OCTET * GROUP_USERS, mix_lanes), bf16),
            pltpu.VMEM((2, blocks, width, lanes), f32),
            pltpu.VMEM((slots, width), f32),
        ],
        compiler_params=pltpu.CompilerParams(vmem_limit_bytes=VMEM_BYTES),
    )(meta, fetched, bilinear, bilt, owner, slot, lens, logits, cot)
    capsules = jnp.dot(select.astype(bf16), out.reshape(blocks * lanes, width), preferred_element_type=f32)
    return capsules.astype(bf16).reshape(blocks * users, interests, width), slot_grads


def fetch_kernel(wanted_ref, table_ref, out_ref, staged, table32, rows32, sems):
    parts = sems.shape[0]
    part = table_ref.shape[0] // parts
    copies = [
        pltpu.make_async_copy(table_ref.at[pl.ds(p * part, part), :], staged.at[pl.ds(p * part, part), :], sems.at[p])
        for p in range(parts)
    ]
    for copy in copies:
        copy.start()
    for p in range(parts):
        copies[p].wait()

        def widen(i, carry):
            base = pl.multiple_of(p * part + i * 128, 128)
            table32[pl.ds(base, 128), :] = staged[pl.ds(base, 128), :].astype(f32)
            return carry

        lax.fori_loop(0, part // 128, widen, 0)

    def copy_rows(i, carry):
        base = pl.multiple_of(i * 8, 8)
        rows = [table32[pl.ds(wanted_ref[base + j], 1), :] for j in range(8)]
        rows32[pl.ds(base, 8), :] = jnp.concatenate(rows, axis=0)
        return carry

    lax.fori_loop(0, out_ref.shape[0] // 8, copy_rows, 0, unroll=2)
    out_ref[...] = rows32[...].astype(bf16)


def fetch_rows(table, wanted):
    table_rows, width = table.shape
    count = wanted.shape[0]
    return pl.pallas_call(
        fetch_kernel,
        out_shape=jax.ShapeDtypeStruct((count, width), bf16),
        in_specs=[pl.BlockSpec(memory_space=pltpu.SMEM), pl.BlockSpec(memory_space=pl.ANY)],
        scratch_shapes=[
            pltpu.VMEM((table_rows, width), bf16),
            pltpu.VMEM((table_rows, width), f32),
            pltpu.VMEM((count, width), f32),
            pltpu.SemaphoreType.DMA((COPIES,)),
        ],
        compiler_params=pltpu.CompilerParams(vmem_limit_bytes=VMEM_BYTES),
    )(wanted, table)


def table_kernel(target_ref, rows_ref, out_ref, acc, sems):
    count = rows_ref.shape[0]
    parts = sems.shape[0]
    part = out_ref.shape[0] // parts
    acc[...] = jnp.zeros_like(acc)

    def step(i, carry):
        base = pl.multiple_of(i * 16, 16)
        rows = rows_ref[pl.ds(base, 16), :].astype(f32)
        where = [target_ref[base + j] for j in range(16)]
        for q in range(0, 16, GROUP_ROWS):
            sums = [acc[pl.ds(where[j], 1), :] + rows[j:j + 1, :] for j in range(q, q + GROUP_ROWS)]
            for j in range(q, q + GROUP_ROWS):
                acc[pl.ds(where[j], 1), :] = sums[j - q]
        return carry

    lax.fori_loop(0, count // 16, step, 0, unroll=2)
    copies = [
        pltpu.make_async_copy(acc.at[pl.ds(p * part, part), :], out_ref.at[pl.ds(p * part, part), :], sems.at[p])
        for p in range(parts)
    ]
    for copy in copies:
        copy.start()
    for copy in copies:
        copy.wait()


def add_to_table(returned, wanted, table_rows):
    count, width = returned.shape
    spare = table_rows + lax.rem(lax.broadcasted_iota(jnp.int32, (count,), 0), GROUP_ROWS)
    targets = jnp.where(wanted >= 0, wanted, spare)
    return pl.pallas_call(
        table_kernel,
        out_shape=jax.ShapeDtypeStruct((table_rows, width), f32),
        in_specs=[pl.BlockSpec(memory_space=pltpu.SMEM), pl.BlockSpec(memory_space=pltpu.VMEM)],
        out_specs=pl.BlockSpec(memory_space=pl.ANY),
        scratch_shapes=[
            pltpu.VMEM((table_rows + GROUP_ROWS, width), f32),
            pltpu.SemaphoreType.DMA((COPIES,)),
        ],
        compiler_params=pltpu.CompilerParams(vmem_limit_bytes=VMEM_BYTES),
    )(targets, returned)


def exchange(x):
    return lax.all_to_all(x, AXES, split_axis=0, concat_axis=0, tiled=True)


def local(item_table, bilinear, requests, history, lengths, init_logits, interest_grad):
    asked_ids = requests[0]
    owner_count, slot_count = asked_ids.shape
    local_table_rows, width = item_table.shape
    wanted = exchange(asked_ids)
    found = fetch_rows(item_table, jnp.maximum(wanted, 0).reshape(-1))
    found, history, lengths, init_logits, interest_grad, bilinear = lax.optimization_barrier(
        (found, history, lengths, init_logits, interest_grad, bilinear))
    fetched = exchange(found.reshape(owner_count, slot_count, width)).reshape(owner_count * slot_count, width)
    prepared = prepare(history, lengths, init_logits, interest_grad, slot_count)
    capsules, slot_grads = route(fetched, bilinear, prepared, slot_count)
    returned = exchange(slot_grads.reshape(owner_count, slot_count, width)).reshape(owner_count * slot_count, width)
    table_grad = add_to_table(returned, wanted.reshape(-1), local_table_rows)
    return capsules, table_grad


def solution(mesh):
    placed = (
        P(AXES, None),
        P(),
        P(AXES, None, None),
        P(AXES, None),
        P(AXES),
        P(AXES, None, None),
        P(AXES, None, None),
    )
    return jax.shard_map(
        local,
        mesh=mesh,
        in_specs=placed,
        out_specs=(P(AXES, None, None), P(AXES, None)),
        check_vma=False,
    )
```

```python
import functools

import jax
import jax.numpy as jnp
from jax import lax
from jax.experimental import pallas as pl
from jax.experimental.pallas import tpu as pltpu
from jax.sharding import PartitionSpec as P

ITERS = 3
squash_eps = 1e-06
AXES = ("gx", "gy")
BLOCK_USERS = 64
TILE_POSITIONS = 4
GROUP_USERS = 16
GROUP_ROWS = 8
COPIES = 8
OCTET = 8
PAIRS = 7
VMEM_BYTES = 60 * 1024 * 1024
f32 = jnp.float32
bf16 = jnp.bfloat16


def dot(a, b):
    return jnp.dot(a, b, preferred_element_type=f32)


def routing_kernel(
    interest_count,
    meta_ref, fetched_ref, bil_ref, bilt_ref, owner_ref, slot_ref, lens_ref, logit_ref, cot_ref,
    interests_ref, slotgrad_ref,
    fetched_t, gram, x_ref, xt_ref, lo_ref, oht_a, oht_b, mix, vecs, vcat, stack, oh_rows,
    sums, logit_now, p_ref, coefs, mix_g, z_ref, slot_acc,
):
    slots, width = fetched_ref.shape
    lanes = owner_ref.shape[2]
    blocks = interests_ref.shape[0]
    pair_max = xt_ref.shape[0]
    pair_rows = xt_ref.shape[2]
    cap = lo_ref.shape[1]
    owners = slots // cap
    users = lanes // interest_count
    groups = users // GROUP_USERS
    group_lanes = lanes // groups
    chunk = oh_rows.shape[0]
    mix_lanes = mix_g.shape[2]
    chunk_count = meta_ref[2 * pair_max]

    for c in range(0, slots, 256):
        fetched_t[:, c:c + 256] = fetched_ref[c:c + 256, :].T
    for k in range(interest_count):
        part = bil_ref[:, k * width:(k + 1) * width]
        gram[:, k * width:(k + 1) * width] = lax.dot_general(
            part, part, (((1,), (1,)), ((), ())), preferred_element_type=f32).astype(bf16)
    slot_acc[...] = jnp.zeros_like(slot_acc)
    vcat[...] = jnp.zeros_like(vcat)
    vecs[...] = jnp.zeros_like(vecs)

    slot_iota = lax.broadcasted_iota(jnp.int32, (cap, lanes), 0)

    def col_user(lane):
        return (lane // group_lanes) * GROUP_USERS + lane % GROUP_USERS

    diag = col_user(lax.broadcasted_iota(jnp.int32, (users, lanes), 1)) == lax.broadcasted_iota(jnp.int32, (users, lanes), 0)
    lane_k = (lax.broadcasted_iota(jnp.int32, (width, lanes), 1) // GROUP_USERS) % interest_count
    half_lane = lax.broadcasted_iota(jnp.int32, (OCTET, 128), 1)
    diag_g = (lax.broadcasted_iota(jnp.int32, (GROUP_USERS, mix_lanes), 1) % GROUP_USERS
              == lax.broadcasted_iota(jnp.int32, (GROUP_USERS, mix_lanes), 0))
    pos_iota = lax.broadcasted_iota(jnp.int32, (OCTET, lanes), 0)

    def place(i):
        return meta_ref[i], meta_ref[pair_max + i]

    def flat(i):
        return pl.ds(pl.multiple_of(i * OCTET, OCTET), OCTET)

    def pair_at(i):
        return pl.ds(pl.multiple_of(i * pair_rows, pair_rows), pair_rows)

    def indicator(orow16, o):
        return jnp.where(orow16 == o, 1.0, 0.0).astype(bf16)

    def over_interests(v):
        parts = []
        for h in range(0, lanes, 128):
            s = v[:, h:h + 128]
            step = group_lanes // 2
            while step >= GROUP_USERS:
                low = half_lane % (2 * step) < step
                s = s + jnp.where(low, pltpu.roll(s, 128 - step, 1), pltpu.roll(s, step, 1))
                step //= 2
            parts.append(s)
        return jnp.concatenate(parts, axis=1)

    def softmax(v):
        e = jnp.exp(v)
        return e / over_interests(e)

    def by_interest(b, mat_ref, v):
        zero = jnp.zeros_like(v)
        for k in range(interest_count):
            stack[b, k * width:(k + 1) * width, :] = jnp.where(lane_k == k, v, zero).astype(bf16)
        return dot(mat_ref[...], stack[b])

    def squash_parts(n):
        root = jnp.sqrt(n + squash_eps)
        fac = root / (1.0 + n)
        slope = (0.5 * (1.0 + n) / root - root) / ((1.0 + n) * (1.0 + n))
        return fac, 2.0 * slope

    def keep_vec(b, vec_t, j):
        vb = vec_t.astype(bf16)
        vecs[b] = vb
        vn = vb.T
        for g in range(groups):
            vcat[b, g, j * group_lanes:(j + 1) * group_lanes, :] = vn[g * group_lanes:(g + 1) * group_lanes, :]

    def build(i, j, buf):
        b, o8 = place(i)
        row = 2 * o8 + j
        crow = slot_ref[b, pl.ds(row, 1), :]
        orow16 = jnp.broadcast_to(owner_ref[b, pl.ds(row, 1), :], (16, lanes))
        lo = jnp.where(slot_iota == crow, 1.0, 0.0).astype(bf16)
        lo_ref[2 * i + j] = lo
        lo3 = lo.reshape(cap // 16, 16, lanes)
        for o in range(owners):
            buf[o * cap:(o + 1) * cap, :] = (lo3 * indicator(orow16, o)[None]).reshape(cap, lanes)

    def gather(i, j, buf):
        xtb = dot(fetched_t[...], buf[...]).astype(bf16)
        xt_ref[i, :, j * lanes:(j + 1) * lanes] = xtb
        start = pl.multiple_of(i * pair_rows + j * lanes, lanes)
        x_ref[pl.ds(start, lanes), :] = xtb.T

    pairs = chunk_count * PAIRS
    build(0, 0, oht_a)

    def gather_pair(i, carry):
        build(i, 1, oht_b)
        gather(i, 0, oht_a)
        build(jnp.minimum(i + 1, pairs - 1), 0, oht_a)
        gather(i, 1, oht_b)
        return carry

    lax.fori_loop(0, pairs, gather_pair, 0)

    def over_pairs(body):
        sums[...] = jnp.zeros_like(sums)

        def step(c, carry):
            work = []
            for q in range(PAIRS):
                i = c * PAIRS + q
                b, o8 = place(i)
                live = pos_iota + o8 * OCTET < lens_ref[pl.ds(b, 1), :]
                work.append((i, b, o8, live))
            coef = body(work)
            for q, (i, b, o8, live) in enumerate(work):
                for l in range(OCTET):
                    row = jnp.broadcast_to(coef[q][l:l + 1, :], (users, lanes))
                    mix[q, l * users:(l + 1) * users, :] = jnp.where(diag, row, 0.0).astype(bf16)
            for q, (i, b, o8, live) in enumerate(work):
                sums[b] += dot(xt_ref[i], mix[q])
            return carry

        lax.fori_loop(0, chunk_count, step, 0)

    def agreement(i, b, live):
        rows = []
        prod = dot(x_ref[pair_at(i), :], vecs[b])
        for l in range(OCTET):
            part = jnp.where(diag, prod[l * users:(l + 1) * users, :], 0.0)
            rows.append(jnp.sum(part, axis=0, keepdims=True))
        return jnp.where(live, jnp.concatenate(rows, axis=0), 0.0)

    def weigh(i, live, logits, j):
        p = softmax(logits)
        if j > 0:
            p_ref[j - 1, flat(i), :] = p
        w = jnp.where(live, p, 0.0)
        coefs[j, flat(i), :] = w
        return w

    def first(work):
        out = []
        for i, b, o8, live in work:
            logits = logit_ref[b, flat(o8), :]
            logit_now[flat(i), :] = logits
            out.append(weigh(i, live, logits, 0))
        return out

    def later(j):
        def body(work):
            out = []
            agreed = [agreement(i, b, live) for i, b, o8, live in work]
            for a, (i, b, o8, live) in zip(agreed, work):
                logits = logit_now[flat(i), :] + a
                if j == 1:
                    logit_now[flat(i), :] = logits
                out.append(weigh(i, live, logits, j))
            return out
        return body

    def back(j_prob, j_coef, j_later):
        def body(work):
            out = []
            agreed = [agreement(i, b, live) for i, b, o8, live in work]
            for dp, (i, b, o8, live) in zip(agreed, work):
                p = p_ref[j_prob, flat(i), :]
                dl = p * (dp - over_interests(p * dp))
                if j_later is not None:
                    dl = dl + coefs[j_later, flat(i), :]
                dl = jnp.where(live, dl, 0.0)
                coefs[j_coef, flat(i), :] = dl
                out.append(dl)
            return out
        return body

    squashed = [None, None]

    def turn(j):
        parts = []
        for b in range(blocks):
            xs = sums[b]
            z = by_interest(b, gram, xs)
            n = jnp.maximum(jnp.sum(xs * z, axis=0, keepdims=True), 0.0)
            fac, slope = squash_parts(n)
            z_ref[j, b] = z
            keep_vec(b, z * fac, 3 + j)
            parts.append((fac, slope))
        squashed[j] = parts

    def turn_back(j):
        for b in range(blocks):
            dxs = sums[b]
            y = by_interest(b, gram, dxs)
            z = z_ref[j, b]
            fac, slope = squashed[j][b]
            inner = slope * jnp.sum(dxs * z, axis=0, keepdims=True)
            keep_vec(b, y * fac + z * inner, j)

    over_pairs(first)
    turn(0)
    over_pairs(later(1))
    turn(1)
    over_pairs(later(2))
    outs = [by_interest(b, bilt_ref, sums[b]) for b in range(blocks)]
    cots = []
    for b, s3 in enumerate(outs):
        fac3, slope3 = squash_parts(jnp.sum(s3 * s3, axis=0, keepdims=True))
        interests_ref[b] = (s3 * fac3).astype(bf16).T
        dc3 = cot_ref[b]
        cots.append(dc3 * fac3 + s3 * (slope3 * jnp.sum(dc3 * s3, axis=0, keepdims=True)))
    for b, ds3 in enumerate(cots):
        keep_vec(b, by_interest(b, bil_ref, ds3), 2)
    over_pairs(back(1, 4, None))
    turn_back(1)
    over_pairs(back(0, 3, 4))
    turn_back(0)

    def row_grads(c, carry):
        for q in range(PAIRS):
            i = c * PAIRS + q
            b, o8 = place(i)
            for g in range(groups):
                src = (g * group_lanes) // 128 * 128
                odd = (g * group_lanes) % 128

                def piece(j, dest):
                    x = coefs[j, flat(i), src:src + 128]
                    return x if odd == dest else pltpu.roll(x, 64, 1)

                parts = []
                for h in range(0, 5, 2):
                    high = piece(h + 1, 64) if h + 1 < 5 else jnp.zeros((OCTET, 128), f32)
                    parts.append(jnp.where(half_lane < 64, piece(h, 0), high))
                row8 = jnp.concatenate(parts, axis=1)
                for l in range(OCTET):
                    row = jnp.broadcast_to(row8[l:l + 1, :], (GROUP_USERS, mix_lanes))
                    mix_g[q * groups + g, l * GROUP_USERS:(l + 1) * GROUP_USERS, :] = (
                        jnp.where(diag_g, row, 0.0).astype(bf16))
        for q in range(PAIRS):
            i = c * PAIRS + q
            b, o8 = place(i)
            for g in range(groups):
                grads = dot(mix_g[q * groups + g], vcat[b, g]).astype(bf16)
                for l in range(OCTET):
                    start = pl.multiple_of(i * pair_rows + (l * users + g * GROUP_USERS), GROUP_USERS)
                    x_ref[pl.ds(start, GROUP_USERS), :] = grads[l * GROUP_USERS:(l + 1) * GROUP_USERS, :]
        return carry

    lax.fori_loop(0, chunk_count, row_grads, 0)

    def scatter(c, carry):
        def slot_chunk(s, carry):
            for q in range(PAIRS):
                i = c * PAIRS + q
                b, o8 = place(i)
                for j in range(2):
                    lo3 = lo_ref[2 * i + j].reshape(cap // 16, 16, lanes)
                    orow16 = jnp.broadcast_to(owner_ref[b, pl.ds(2 * o8 + j, 1), :], (16, lanes))
                    t = 2 * q + j
                    for oo in range(chunk // cap):
                        ind = indicator(orow16, s * (chunk // cap) + oo)
                        oh_rows[oo * cap:(oo + 1) * cap, t * lanes:(t + 1) * lanes] = (
                            lo3 * ind[None]).reshape(cap, lanes)
            start = pl.multiple_of(s * chunk, chunk)
            rows = pl.ds(pl.multiple_of(c * PAIRS * pair_rows, PAIRS * pair_rows), PAIRS * pair_rows)
            slot_acc[pl.ds(start, chunk), :] += dot(oh_rows[...], x_ref[rows, :])
            return carry

        return lax.fori_loop(0, slots // chunk, slot_chunk, carry)

    lax.fori_loop(0, chunk_count, scatter, 0)
    slotgrad_ref[...] = slot_acc[...].astype(bf16)


def prepare(history, lengths, init_logits, interest_grad, cap):
    users, hist_count = history.shape
    interests = init_logits.shape[2]
    width = interest_grad.shape[2]
    lanes = interests * BLOCK_USERS
    blocks = users // BLOCK_USERS
    octets = -(-hist_count // OCTET)
    positions = octets * OCTET
    index = lax.iota(jnp.int32, users)
    ahead = (lengths[None, :] > lengths[:, None]) | (
        (lengths[None, :] == lengths[:, None]) & (index[None, :] < index[:, None]))
    rank = jnp.sum(ahead.astype(jnp.int32), axis=1)
    order = (rank[:, None] == index[None, :]).astype(bf16)
    column = lax.iota(jnp.int32, users * interests)
    block, rest = column // lanes, column % lanes
    group_lanes = interests * GROUP_USERS
    user = block * BLOCK_USERS + rest // group_lanes * GROUP_USERS + rest % GROUP_USERS
    interest = rest // GROUP_USERS % interests
    select = ((rank[:, None, None] == user[None, None, :])
              & (lax.iota(jnp.int32, interests)[None, :, None] == interest[None, None, :]))
    select = select.reshape(users * interests, users * interests)
    by_k = ((rank[None, :, None] == user[None, None, :])
            & (lax.iota(jnp.int32, interests)[:, None, None] == interest[None, None, :]))
    by_k = by_k.reshape(users * interests, users * interests)

    def sort_positions(values):
        s = jnp.dot(values.astype(bf16).T, order, preferred_element_type=f32).astype(jnp.int32)
        s = jnp.pad(s, ((0, positions - hist_count), (0, 0)))
        s = s.reshape(positions // TILE_POSITIONS, TILE_POSITIONS, blocks, BLOCK_USERS).transpose(2, 0, 1, 3)
        s = s.reshape(blocks, positions // TILE_POSITIONS, TILE_POSITIONS * BLOCK_USERS)
        return jnp.pad(s, ((0, 1), (0, 0), (0, 0)))

    owner = sort_positions(history // cap)
    slot = sort_positions(history % cap)
    sorted_lens = jnp.sum(jnp.where(rank[:, None] == index[None, :], lengths[:, None], 0), axis=0)
    need = (sorted_lens[::BLOCK_USERS] + OCTET - 1) // OCTET
    upto = jnp.sum(jnp.where(lax.iota(jnp.int32, blocks)[None, :] <= lax.iota(jnp.int32, blocks)[:, None], need[None, :], 0), axis=1)
    pair_max = -(-blocks * octets // PAIRS) * PAIRS
    pair = lax.iota(jnp.int32, pair_max)
    passed = pair[:, None] >= upto[None, :]
    pair_block = jnp.sum(passed.astype(jnp.int32), axis=1)
    pair_octet = jnp.where(pair_block < blocks, pair - jnp.sum(jnp.where(passed, need[None, :], 0), axis=1), 0)
    chunks = (jnp.sum(need) + PAIRS - 1) // PAIRS
    meta = jnp.concatenate([pair_block, pair_octet, chunks[None]])
    lens = jnp.sum(jnp.where(rank[:, None] == user[None, :], lengths[:, None], 0), axis=0).reshape(blocks, lanes)
    lens = jnp.pad(lens, ((0, 1), (0, 0)))
    flat = init_logits.transpose(1, 2, 0).reshape(hist_count, interests * users)
    logits = jnp.dot(flat, by_k.astype(f32), precision=lax.Precision.HIGHEST, preferred_element_type=f32)
    logits = jnp.pad(logits, ((0, positions - hist_count), (0, lanes))).reshape(positions, blocks + 1, lanes).transpose(1, 0, 2)
    grads = interest_grad.reshape(users * interests, width)
    cot = lax.dot_general(grads.astype(bf16), select.astype(bf16), (((0,), (0,)), ((), ())), preferred_element_type=f32)
    cot = cot.reshape(width, blocks, lanes).transpose(1, 0, 2)
    return owner, slot, meta, lens, logits, cot, select


def route(fetched, bilinear, prepared, cap):
    owner, slot, meta, lens, logits, cot, select = prepared
    slots, width = fetched.shape
    blocks, _, lanes = cot.shape
    interests = bilinear.shape[1] // width
    users = lanes // interests
    groups = users // GROUP_USERS
    pair_max = (meta.shape[0] - 1) // 2
    pair_rows = OCTET * users
    mix_lanes = -(-5 * lanes // groups // 128) * 128
    bilt = bilinear.reshape(width, interests, width).transpose(2, 1, 0).reshape(width, interests * width)
    chunk = 1024 if slots <= 2048 else 512
    out, slot_grads = pl.pallas_call(
        functools.partial(routing_kernel, interests),
        out_shape=(
            jax.ShapeDtypeStruct((blocks, lanes, width), bf16),
            jax.ShapeDtypeStruct((slots, width), bf16),
        ),
        in_specs=[pl.BlockSpec(memory_space=pltpu.SMEM)] + [pl.BlockSpec(memory_space=pltpu.VMEM)] * 8,
        scratch_shapes=[
            pltpu.VMEM((width, slots), bf16),
            pltpu.VMEM((width, interests * width), bf16),
            pltpu.VMEM((pair_max * pair_rows, width), bf16),
            pltpu.VMEM((pair_max, width, pair_rows), bf16),
            pltpu.VMEM((pair_max * 2, cap, lanes), bf16),
            pltpu.VMEM((slots, lanes), bf16),
            pltpu.VMEM((slots, lanes), bf16),
            pltpu.VMEM((PAIRS, pair_rows, lanes), bf16),
            pltpu.VMEM((blocks + 1, width, lanes), bf16),
            pltpu.VMEM((blocks + 1, groups, mix_lanes, width), bf16),
            pltpu.VMEM((blocks, interests * width, lanes), bf16),
            pltpu.VMEM((chunk, PAIRS * pair_rows), bf16),
            pltpu.VMEM((blocks + 1, width, lanes), f32),
            pltpu.VMEM((pair_max * OCTET, lanes), f32),
            pltpu.VMEM((2, pair_max * OCTET, lanes), f32),
            pltpu.VMEM((5, pair_max * OCTET, lanes), f32),
            pltpu.VMEM((PAIRS * groups, OCTET * GROUP_USERS, mix_lanes), bf16),
            pltpu.VMEM((2, blocks, width, lanes), f32),
            pltpu.VMEM((slots, width), f32),
        ],
        compiler_params=pltpu.CompilerParams(vmem_limit_bytes=VMEM_BYTES),
    )(meta, fetched, bilinear, bilt, owner, slot, lens, logits, cot)
    capsules = jnp.dot(select.astype(bf16), out.reshape(blocks * lanes, width), preferred_element_type=f32)
    return capsules.astype(bf16).reshape(blocks * users, interests, width), slot_grads


def fetch_kernel(wanted_ref, table_ref, out_ref, staged, table32, rows32, sems):
    parts = sems.shape[0]
    part = table_ref.shape[0] // parts
    copies = [
        pltpu.make_async_copy(table_ref.at[pl.ds(p * part, part), :], staged.at[pl.ds(p * part, part), :], sems.at[p])
        for p in range(parts)
    ]
    for copy in copies:
        copy.start()
    for p in range(parts):
        copies[p].wait()

        def widen(i, carry):
            base = pl.multiple_of(p * part + i * 128, 128)
            table32[pl.ds(base, 128), :] = staged[pl.ds(base, 128), :].astype(f32)
            return carry

        lax.fori_loop(0, part // 128, widen, 0)

    def copy_rows(i, carry):
        base = pl.multiple_of(i * 8, 8)
        rows = [table32[pl.ds(wanted_ref[base + j], 1), :] for j in range(8)]
        rows32[pl.ds(base, 8), :] = jnp.concatenate(rows, axis=0)
        return carry

    lax.fori_loop(0, out_ref.shape[0] // 8, copy_rows, 0, unroll=2)
    out_ref[...] = rows32[...].astype(bf16)


def fetch_rows(table, wanted):
    table_rows, width = table.shape
    count = wanted.shape[0]
    return pl.pallas_call(
        fetch_kernel,
        out_shape=jax.ShapeDtypeStruct((count, width), bf16),
        in_specs=[pl.BlockSpec(memory_space=pltpu.SMEM), pl.BlockSpec(memory_space=pl.ANY)],
        scratch_shapes=[
            pltpu.VMEM((table_rows, width), bf16),
            pltpu.VMEM((table_rows, width), f32),
            pltpu.VMEM((count, width), f32),
            pltpu.SemaphoreType.DMA((COPIES,)),
        ],
        compiler_params=pltpu.CompilerParams(vmem_limit_bytes=VMEM_BYTES),
    )(wanted, table)


def table_kernel(target_ref, rows_ref, out_ref, acc, sems):
    count = rows_ref.shape[0]
    parts = sems.shape[0]
    part = out_ref.shape[0] // parts
    acc[...] = jnp.zeros_like(acc)

    def step(i, carry):
        base = pl.multiple_of(i * 16, 16)
        rows = rows_ref[pl.ds(base, 16), :].astype(f32)
        where = [target_ref[base + j] for j in range(16)]
        for q in range(0, 16, GROUP_ROWS):
            sums = [acc[pl.ds(where[j], 1), :] + rows[j:j + 1, :] for j in range(q, q + GROUP_ROWS)]
            for j in range(q, q + GROUP_ROWS):
                acc[pl.ds(where[j], 1), :] = sums[j - q]
        return carry

    lax.fori_loop(0, count // 16, step, 0, unroll=2)
    copies = [
        pltpu.make_async_copy(acc.at[pl.ds(p * part, part), :], out_ref.at[pl.ds(p * part, part), :], sems.at[p])
        for p in range(parts)
    ]
    for copy in copies:
        copy.start()
    for copy in copies:
        copy.wait()


def add_to_table(returned, wanted, table_rows):
    count, width = returned.shape
    spare = table_rows + lax.rem(lax.broadcasted_iota(jnp.int32, (count,), 0), GROUP_ROWS)
    targets = jnp.where(wanted >= 0, wanted, spare)
    return pl.pallas_call(
        table_kernel,
        out_shape=jax.ShapeDtypeStruct((table_rows, width), f32),
        in_specs=[pl.BlockSpec(memory_space=pltpu.SMEM), pl.BlockSpec(memory_space=pltpu.VMEM)],
        out_specs=pl.BlockSpec(memory_space=pl.ANY),
        scratch_shapes=[
            pltpu.VMEM((table_rows + GROUP_ROWS, width), f32),
            pltpu.SemaphoreType.DMA((COPIES,)),
        ],
        compiler_params=pltpu.CompilerParams(vmem_limit_bytes=VMEM_BYTES),
    )(targets, returned)


def exchange(x):
    return lax.all_to_all(x, AXES, split_axis=0, concat_axis=0, tiled=True)


def local(item_table, bilinear, requests, history, lengths, init_logits, interest_grad):
    asked_ids = requests[0]
    owner_count, slot_count = asked_ids.shape
    local_table_rows, width = item_table.shape
    wanted = exchange(asked_ids)
    found = fetch_rows(item_table, jnp.maximum(wanted, 0).reshape(-1))
    found, history, init_logits, interest_grad, bilinear = lax.optimization_barrier(
        (found, history, init_logits, interest_grad, bilinear))
    fetched = exchange(found.reshape(owner_count, slot_count, width)).reshape(owner_count * slot_count, width)
    prepared = prepare(history, lengths, init_logits, interest_grad, slot_count)
    capsules, slot_grads = route(fetched, bilinear, prepared, slot_count)
    returned = exchange(slot_grads.reshape(owner_count, slot_count, width)).reshape(owner_count * slot_count, width)
    table_grad = add_to_table(returned, wanted.reshape(-1), local_table_rows)
    return capsules, table_grad


def solution(mesh):
    placed = (
        P(AXES, None),
        P(),
        P(AXES, None, None),
        P(AXES, None),
        P(AXES),
        P(AXES, None, None),
        P(AXES, None, None),
    )
    return jax.shard_map(
        local,
        mesh=mesh,
        in_specs=placed,
        out_specs=(P(AXES, None, None), P(AXES, None)),
        check_vma=False,
    )
```
